32 devices in a mesh: dp: 8 (over z, x), tensor: 4 (over y, core).
Axes of the slice: x: 2, y: 2, z: 4, core: 2. Of those that a mesh axis runs over, the one named last changes fastest.
Arguments:
- tokens: bfloat16 [2048, 8192], P('dp', 'tensor'), may hold values from -6 to 6
- block_routing: int32 [8, 2], replicated, may hold values from -1 to 7, as said below
- frozen_up_weight: bfloat16 [8192, 28672], P('tensor', 'dp'), may hold values from -0.0625 to 0.0625
- adapter_down_weight: bfloat16 [32, 8192], P(None, 'tensor'), may hold values from -0.0625 to 0.0625
- adapter_up_weight: bfloat16 [32, 28672], P(None, 'dp'), may hold values from -6 to 6
- magnitude: float32 [28672], P('dp'), may hold values from 0.5 to 2
- cotangent: bfloat16 [1024, 28672], P('tensor', 'dp'), may hold values from -6 to 6
Outputs:
- projected: bfloat16 [1024, 28672], P('tensor', 'dp')
- grad_a: float32 [32, 8192], P(None, 'tensor')
- grad_b: float32 [32, 28672], P(None, 'dp')
- grad_m: float32 [28672], P('dp')
The draws below stay inside these ranges and needn't reach their ends.
Inputs may be any that keep to these rules, and one draw needn't show every extreme that they name: `block_routing`: row d lists where the two blocks of dp index d go. Live blocks come first and -1 marks a padding block. A first live block stays on its own index; a second live block goes to index (d + half the dp size) mod the dp size, which then has no live block. Every dp index receives exactly one block. In every draw some index has two live blocks and some has none.
All inputs are finite; a program needn't handle non-finite values.
Results may differ from the reference program's by a relative error of at most 0.018.
Values may be sent and summed in bfloat16 or wider, within the bound.
A program may use at most 128 MiB of HBM per device.

```python
import math
import jax
import jax.numpy as jnp
from jax import lax

MODEL_WIDTH = 8192
HIDDEN_UNITS = 28672
ADAPTER_RANK = 32
SLOTS = 2
BLK = 128
T_LIVE = 1024
N_DP = 8
N_TENSOR = 4


def draw_block_routing(key, part):
    half_count = N_DP // 2
    key_kind, key_pick, key_force = jax.random.split(key, 3)
    kinds = jax.random.randint(key_kind, (half_count,), 0, 3)
    chosen = jax.random.randint(key_pick, (), 0, half_count)
    forced = 1 + jax.random.randint(key_force, (), 0, 2)
    kinds = jnp.where(jnp.arange(half_count) == chosen, forced, kinds)
    lower_counts = jnp.where(kinds == 0, 1, jnp.where(kinds == 1, 2, 0))
    counts = jnp.concatenate([lower_counts, 2 - lower_counts])
    devices = jnp.arange(N_DP, dtype=jnp.int32)
    partner = (devices + half_count) % N_DP
    first_slot = jnp.where(counts >= 1, devices, -1)
    second_slot = jnp.where(counts == 2, partner, -1)
    return jnp.stack([first_slot, second_slot], axis=1).astype(jnp.int32)


def level_of(stream_key, shape, cuts, least, high):
    def one(position, parts):
        steps = jax.random.uniform(jax.random.fold_in(jax.random.fold_in(stream_key, 6), position), (parts,), jnp.float32, least / len(cuts), high / len(cuts))
        return jnp.repeat(jnp.exp(steps), shape[position] // parts).reshape((-1,) + (1,) * (len(shape) - position - 1))

    level = one(*cuts[0])
    for cut in cuts[1:]:
        level = level * one(*cut)
    return level


def scatter_about(stream_key, shape, deviation, most, cuts=(), kind=jnp.bfloat16):
    loudness = level_of(stream_key, shape, cuts, -0.22, 0.18) if cuts else 1.0
    result = jax.random.normal(stream_key, shape, jnp.float32) * deviation * loudness
    return jnp.minimum(jnp.maximum(result, -most), most).astype(kind)


def setup_inputs(seed: int = 0) -> dict:
    keys = jax.random.split(jax.random.key(seed), 8)
    return {
        "tokens": scatter_about(keys[0], (N_DP * SLOTS * BLK, MODEL_WIDTH), 1.0, 6.0, ((0, 8), (1, 4))),
        "block_routing": draw_block_routing(jax.random.fold_in(keys[7], 71), 0),
        "frozen_up_weight": scatter_about(keys[2], (MODEL_WIDTH, HIDDEN_UNITS), MODEL_WIDTH ** -0.5, 0.0625, ((0, 4), (1, 8))),
        "adapter_down_weight": scatter_about(keys[3], (ADAPTER_RANK, MODEL_WIDTH), MODEL_WIDTH ** -0.5, 0.0625, ((1, 4),)),
        "adapter_up_weight": scatter_about(keys[4], (ADAPTER_RANK, HIDDEN_UNITS), 1.0, 6.0, ((1, 8),)),
        "magnitude": jnp.clip(jnp.exp(math.log(2.0) - 1.3862944 * jax.random.uniform(keys[5], (HIDDEN_UNITS,), jnp.float32) ** level_of(keys[5], (HIDDEN_UNITS,), ((0, 8),), -0.2, 0.2)), 0.5, 2.0),
        "cotangent": scatter_about(keys[6], (T_LIVE, HIDDEN_UNITS), 1.0, 6.0, ((0, 4), (1, 8))),
    }


def contract_dims(left, right, left_dim, right_dim):
    return lax.dot_general(left, right, (((left_dim,), (right_dim,)), ((), ())), preferred_element_type=jnp.float32)

def reference(tokens, block_routing, frozen_up_weight, adapter_down_weight, adapter_up_weight, magnitude, cotangent):
    adapter_scale = 1.0 / math.sqrt(ADAPTER_RANK)
    flat_plan = block_routing.reshape(-1)
    matches = (flat_plan[None, :] == jnp.arange(N_DP, dtype=jnp.int32)[:, None]).astype(jnp.int32)
    source = lax.optimization_barrier(jnp.sum(matches * jnp.arange(N_DP * SLOTS, dtype=jnp.int32)[None, :], axis=1)).astype(jnp.int32)
    blocks = tokens.reshape(N_DP * SLOTS, BLK, MODEL_WIDTH)
    active_tokens = jnp.take(blocks, source, axis=0).reshape(T_LIVE, MODEL_WIDTH)
    group_width = MODEL_WIDTH // N_TENSOR
    frozen_sum = jnp.zeros((T_LIVE, HIDDEN_UNITS), jnp.float32)
    for group_idx in range(N_TENSOR):
        lower = group_idx * group_width
        partial_prod = jnp.dot(active_tokens[:, lower:lower + group_width], frozen_up_weight[lower:lower + group_width, :], preferred_element_type=jnp.float32)
        rounded = lax.optimization_barrier(partial_prod.astype(jnp.bfloat16))
        frozen_sum = frozen_sum + rounded.astype(jnp.float32)
    down_factor_half = contract_dims(active_tokens, adapter_down_weight, 1, 1).astype(jnp.bfloat16)
    column_span = HIDDEN_UNITS // N_DP

    def column_squares(block_position):
        weight_columns = lax.dynamic_slice_in_dim(frozen_up_weight, block_position * column_span, column_span, 1).astype(jnp.float32)
        up_factor_columns = lax.dynamic_slice_in_dim(adapter_up_weight, block_position * column_span, column_span, 1)
        merged_weight = weight_columns + adapter_scale * contract_dims(adapter_down_weight, up_factor_columns, 0, 0)
        return lax.optimization_barrier(jnp.sum(merged_weight * merged_weight, axis=0))
    col_square = lax.map(column_squares, jnp.arange(N_DP, dtype=jnp.int32)).reshape(HIDDEN_UNITS)
    col_norm = jnp.maximum(jnp.sqrt(col_square), 0.5)
    unscaled_output = frozen_sum + adapter_scale * jnp.dot(down_factor_half, adapter_up_weight, preferred_element_type=jnp.float32)
    col_factor = magnitude / col_norm
    projected = (unscaled_output * col_factor).astype(jnp.bfloat16)
    inverse = 1.0 / math.sqrt(T_LIVE)
    cot_full = cotangent.astype(jnp.float32)
    scaled_gradient = (cot_full * col_factor * inverse).astype(jnp.bfloat16)
    grad_m = lax.optimization_barrier(jnp.sum(cot_full * unscaled_output, axis=0)) / col_norm * inverse
    grad_b = adapter_scale * contract_dims(down_factor_half, scaled_gradient, 0, 0)
    row_gradient = contract_dims(scaled_gradient, adapter_up_weight, 1, 1).astype(jnp.bfloat16)
    grad_a = adapter_scale * contract_dims(row_gradient, active_tokens, 0, 0)
    return (projected, grad_a, grad_b, grad_m)
```

```python
import functools
import math

import jax
import jax.numpy as jnp
from jax import lax
from jax.experimental import pallas as pl
from jax.experimental.pallas import tpu as pltpu
from jax.sharding import PartitionSpec as P

BLK = 128
ROWS = 16
CHUNKS = BLK // ROWS
AHEAD = 3
LANES = 128
MESH = pl.DeviceIdType.MESH
F32 = jnp.float32
BF16 = jnp.bfloat16


def mirrored(value, bits):
    result = 0
    for position in range(bits):
        result = result + (value // (1 << position)) % 2 * (1 << (bits - 1 - position))
    return result


def flipped(value, bit):
    return value + bit - 2 * bit * ((value // bit) % 2)


def dots(left, right, left_dim, right_dim):
    return lax.dot_general(
        left, right, (((left_dim,), (right_dim,)), ((), ())), preferred_element_type=F32
    )


def kernel(
    cfg,
    tok_in, routing, w_hbm, down, up, mag, cot,
    out, ga_out, gb_out, gm_out,
    w, raw, tok, part, near, pair, far, downp, sq, sq_near, sq_far, factor, norm, sg,
    rp, rp_in, rgt, rg, proj_down, gm_acc, gb_part, gb_near, gb_sum, gb_far, gm_part, gm_in,
    w_sem, s0_send, s0_recv, st_send, st_recv, nr_send, nr_recv, fr_send, fr_recv, ms_send, ms_recv,
):
    dp, tp, width, cols, rank, tile, tps = cfg
    bits = dp.bit_length() - 1
    per = dp // tp
    tiles = cols // tile
    scale = 1.0 / math.sqrt(rank)
    inverse = 1.0 / math.sqrt(dp * BLK)
    d = lax.axis_index("dp")
    t = lax.axis_index("tensor")
    core = t % 2
    side = t // 2
    t_near, t_far = flipped(t, 1), flipped(t, 2)
    hops = [flipped(d, dp >> (k + 1)) for k in range(bits)]

    def copy(src, dst, send, recv, target):
        return pltpu.make_async_remote_copy(
            src_ref=src, dst_ref=dst, send_sem=send, recv_sem=recv,
            device_id=target, device_id_type=MESH,
        )

    def to_dp(k):
        return {"dp": hops[k]}

    near_id, far_id = {"tensor": t_near}, {"tensor": t_far}

    def w_copy(n):
        at = pl.ds(pl.multiple_of(n * tile, tile), tile)
        return pltpu.make_async_copy(w_hbm.at[:, at], w.at[:, at], w_sem.at[n])

    def first(c):
        return copy(tok_in.at[:, c], raw.at[c], s0_send.at[c], s0_recv.at[c], to_dp(0))

    def stage(k, c, owner):
        size = 1 << k
        base = mirrored(owner, bits) // size * size
        here = tok.at[c, pl.ds(pl.multiple_of(base * ROWS, ROWS), size * ROWS)]
        return copy(here, here, st_send.at[k - 1, c], st_recv.at[k - 1, c], to_dp(k))

    def near_copy(c):
        start = (1 - core) * 2
        return copy(part.at[c, :, pl.ds(start, 2)], near.at[c], nr_send.at[c], nr_recv.at[c], near_id)

    def far_copy(c):
        return copy(pair.at[c], far.at[c], fr_send.at[c], fr_recv.at[c], far_id)

    def small(n, src, dst, target):
        return copy(src, dst, ms_send.at[n], ms_recv.at[n], target)

    sq1 = small(0, sq, sq_near, near_id)
    sq2 = small(1, sq_near, sq_far, far_id)
    rp_hops = [small(2 + k, rp.at[k], rp_in.at[k], to_dp(k)) for k in range(bits)]
    n0 = 2 + bits
    rg1 = small(n0, rgt.at[t], rgt.at[t], near_id)
    rg1_in = small(n0, rgt.at[t_near], rgt.at[t_near], near_id)
    mine2 = pl.ds(side * 2, 2)
    theirs2 = pl.ds((1 - side) * 2, 2)
    rg2 = small(n0 + 1, rgt.at[mine2], rgt.at[mine2], far_id)
    rg2_in = small(n0 + 1, rgt.at[theirs2], rgt.at[theirs2], far_id)

    def each_tile(body):
        @pl.loop(0, tiles)
        def _(n):
            body(pl.ds(pl.multiple_of(n * tile, tile), tile))

    @pl.loop(0, tiles)
    def _(n):
        w_copy(n).start()

    barrier = pltpu.get_barrier_semaphore()
    for k in range(bits):
        pl.semaphore_signal(barrier, inc=1, device_id=to_dp(k), device_id_type=MESH)
    pl.semaphore_signal(barrier, inc=1, device_id=near_id, device_id_type=MESH)
    pl.semaphore_signal(barrier, inc=1, device_id=far_id, device_id_type=MESH)
    pl.semaphore_wait(barrier, bits + 2)

    for c in range(AHEAD):
        first(c).start()
    downp[...] = jnp.zeros_like(downp)
    downp[:rank, :] = down[...]
    gm_acc[...] = jnp.zeros_like(gm_acc)

    own_live = routing[d, 0] == d
    pair_live = routing[hops[0], 0] == hops[0]
    norm_last = (tiles + tps - 1) // tps - 1
    depth = 256

    def norm_tile(n):
        w_copy(n).wait()
        at = pl.ds(pl.multiple_of(n * tile, tile), tile)

        def add(r, total):
            rows = pl.ds(pl.multiple_of(r * depth, depth), depth)
            merged = w[rows, at].astype(F32) + scale * dots(down[:, rows], up[:, at], 0, 0)
            return total + jnp.sum((merged * merged).reshape(depth // 8, 8, tile), axis=0)

        total = lax.fori_loop(0, width // depth, add, jnp.zeros((8, tile), F32))
        sq[:, at] = jnp.sum(total, axis=0, keepdims=True)

    def gradient():
        def body(at):
            square = sq_near[:, at] + sq_far[:, at]
            size = jnp.maximum(jnp.sqrt(square), 0.5)
            ratio = mag[:, at] / size
            norm[:, at] = size
            factor[:, at] = ratio
            for g in range(per):
                sg[g, :, at] = (cot[g, :, at].astype(F32) * ratio * inverse).astype(BF16)

        each_tile(body)
        for g in range(per):
            rp[0, :, g * BLK:(g + 1) * BLK] = dots(up[...], sg[g], 1, 1)
        rp_hops[0].start()

    def epilogue(c):
        mine = core * 2 + side
        rows = pl.ds(pl.multiple_of(c * ROWS, ROWS), ROWS)
        high = per * ROWS

        def total(at, wide):
            return (
                part[c, :, mine, :, at].astype(F32)
                + near[c, :, side, :, at].astype(F32)
                + far[c, :, :, at].astype(F32)
            ).reshape(high, wide)

        small_down = total(pl.ds(cols, LANES), LANES).astype(BF16)
        proj_down[:, rows, :] = small_down.reshape(per, ROWS, LANES)
        lhs = small_down[:, :rank]

        def body(at):
            pre = total(at, tile) + scale * jnp.dot(lhs, up[:, at], preferred_element_type=F32)
            out[:, rows, at] = (pre * factor[:, at]).astype(BF16).reshape(per, ROWS, tile)
            both = cot[:, rows, at].astype(F32).reshape(high, tile) * pre
            gm_acc[:, at] += jnp.sum(both.reshape(high // 8, 8, tile), axis=0)

        each_tile(body)

    def when(condition, action):
        pl.when(condition)(action)

    steps = CHUNKS + bits + 1

    @pl.loop(0, steps)
    def _(i):
        when(i + AHEAD < CHUNKS, lambda: first(i + AHEAD).start())

        @pl.when(i < CHUNKS)
        def _():
            first(i).wait_recv()
            own_at = pl.ds(pl.multiple_of(mirrored(d, bits) * ROWS, ROWS), ROWS)
            pair_at = pl.ds(pl.multiple_of(mirrored(hops[0], bits) * ROWS, ROWS), ROWS)
            tok[i, own_at] = jnp.where(own_live, tok_in[0, i], raw[i, 1])
            tok[i, pair_at] = jnp.where(pair_live, raw[i, 0], tok_in[1, i])
            stage(1, i, d).start()

        for k in range(1, bits):
            j = i - k

            @pl.when((j >= 0) & (j < CHUNKS))
            def _():
                stage(k, j, hops[k]).wait_recv()
                if k < bits - 1:
                    stage(k + 1, j, d).start()

        @pl.when(i <= norm_last)
        def _():
            for e in range(tps):
                n = i * tps + e
                when(n < tiles, lambda: norm_tile(n))

        when(i == norm_last, lambda: sq1.start())

        @pl.when(i == norm_last + 1)
        def _():
            sq1.wait()
            sq_near[...] = sq_near[...] + sq[...]
            sq2.start()

        @pl.when(i == norm_last + 2)
        def _():
            sq2.wait()
            gradient()

        for k in range(bits):
            @pl.when(i == norm_last + 3 + k)
            def _():
                rp_hops[k].wait()
                merged = rp[k] + rp_in[k]
                if k < bits - 1:
                    rp[k + 1] = merged
                    rp_hops[k + 1].start()
                else:
                    rgt[t] = merged.astype(BF16)
                    rg1.start()

        @pl.when(i == norm_last + 3 + bits)
        def _():
            rg1.wait_send()
            rg1_in.wait_recv()
            rg2.start()

        j_near = i - bits

        @pl.when((j_near >= 0) & (j_near < CHUNKS))
        def _():
            near_copy(j_near).wait_recv()
            other = core * 2 + 1 - side

            def body(at):
                pair[j_near, :, :, at] = (
                    part[j_near, :, other, :, at].astype(F32)
                    + near[j_near, :, 1 - side, :, at].astype(F32)
                ).astype(BF16)

            each_tile(body)
            body(pl.ds(cols, LANES))
            far_copy(j_near).start()

        j_mat = i - (bits - 1)

        @pl.when((j_mat >= 0) & (j_mat < CHUNKS))
        def _():
            lhs = tok.at[j_mat]

            def body(at):
                prod = jnp.dot(lhs[...], w[:, at], preferred_element_type=F32)
                part[j_mat, :, :, :, at] = prod.astype(BF16).reshape(per, tp, ROWS, tile)

            each_tile(body)
            part[j_mat, :, :, :, cols:] = (
                dots(lhs[...], downp[...], 1, 1).astype(BF16).reshape(per, tp, ROWS, LANES)
            )
            near_copy(j_mat).start()

        j_far = i - bits - 1

        @pl.when((j_far >= 0) & (j_far < CHUNKS - 1))
        def _():
            far_copy(j_far).wait_recv()
            epilogue(j_far)

    rg2.wait_send()
    rg2_in.wait_recv()
    for s in range(tp):
        turned = rgt[s].astype(F32).T.astype(BF16)
        spot = s % 2 * 2 + s // 2
        for g in range(per):
            for c in range(CHUNKS):
                low = g * BLK + c * ROWS
                rg[c, g, spot] = turned[low:low + ROWS]

    wide = min(512, width)

    @pl.loop(0, width // wide)
    def _(n):
        at = pl.ds(pl.multiple_of(n * wide, wide), wide)

        def add(c, total):
            return total + dots(rg[c].reshape(dp * ROWS, rank), tok[c, :, at], 0, 0)

        ga_out[:, at] = scale * lax.fori_loop(0, CHUNKS, add, jnp.zeros((rank, wide), F32))

    far_copy(CHUNKS - 1).wait_recv()
    epilogue(CHUNKS - 1)

    n1 = n0 + 2
    gb1 = small(n1, gb_part, gb_near, near_id)
    gb2 = small(n1 + 1, gb_sum, gb_far, far_id)
    gm1 = small(n1 + 2, gm_part.at[0], gm_in.at[0], near_id)
    gm2 = small(n1 + 3, gm_part.at[1], gm_in.at[1], far_id)
    live = proj_down[...].reshape(per * BLK, LANES)[:, :rank]

    def ends(at):
        gb_part[:, at] = (
            scale * dots(live, sg[:, :, at].reshape(per * BLK, tile), 0, 0)
        ).astype(BF16)
        gm_part[0, :, at] = (
            jnp.sum(gm_acc[:, at], axis=0, keepdims=True) / norm[:, at] * inverse
        )

    each_tile(ends)
    gm1.start()
    gb1.start()
    gm1.wait()
    gm_part[1] = gm_part[0] + gm_in[0]
    gm2.start()
    gb1.wait()

    def sums(at):
        gb_sum[:, at] = (gb_part[:, at].astype(F32) + gb_near[:, at].astype(F32)).astype(BF16)

    each_tile(sums)
    gb2.start()
    gm2.wait()
    gm_out[...] = gm_part[1] + gm_in[1]
    gb2.wait()

    def last(at):
        gb_out[:, at] = gb_sum[:, at].astype(F32) + gb_far[:, at].astype(F32)

    each_tile(last)

    @pl.loop(0, CHUNKS)
    def _(c):
        first(c).wait_send()
        for k in range(1, bits):
            stage(k, c, d).wait_send()
        near_copy(c).wait_send()
        far_copy(c).wait_send()


def body(dp, tp, tokens, routing, weight, down, up, mag, cot):
    width, cols = weight.shape
    rank = down.shape[0]
    per = dp // tp
    bits = dp.bit_length() - 1
    tile = next(size for size in (512, 256, 128) if cols % size == 0)
    tiles = cols // tile
    tps = -(-tiles // bits)
    cfg = (dp, tp, width, cols, rank, tile, tps)
    ext = cols + LANES
    vmem = pl.BlockSpec(memory_space=pltpu.VMEM)
    dma = pltpu.SemaphoreType.DMA
    mine = per * BLK
    misc = bits + 8
    out, ga, gb, gm = pl.pallas_call(
        functools.partial(kernel, cfg),
        out_shape=(
            jax.ShapeDtypeStruct((per, BLK, cols), BF16),
            jax.ShapeDtypeStruct((rank, width), F32),
            jax.ShapeDtypeStruct((rank, cols), F32),
            jax.ShapeDtypeStruct((1, cols), F32),
        ),
        in_specs=[
            vmem,
            pl.BlockSpec(memory_space=pltpu.SMEM),
            pl.BlockSpec(memory_space=pl.ANY),
            vmem, vmem, vmem, vmem,
        ],
        out_specs=(vmem, vmem, vmem, vmem),
        scratch_shapes=[
            pltpu.VMEM((width, cols), BF16),
            pltpu.VMEM((CHUNKS, 2, ROWS, width), BF16),
            pltpu.VMEM((CHUNKS, dp * ROWS, width), BF16),
            pltpu.VMEM((CHUNKS, per, tp, ROWS, ext), BF16),
            pltpu.VMEM((CHUNKS, per, 2, ROWS, ext), BF16),
            pltpu.VMEM((CHUNKS, per, ROWS, ext), BF16),
            pltpu.VMEM((CHUNKS, per, ROWS, ext), BF16),
            pltpu.VMEM((LANES, width), BF16),
            pltpu.VMEM((1, cols), F32),
            pltpu.VMEM((1, cols), F32),
            pltpu.VMEM((1, cols), F32),
            pltpu.VMEM((1, cols), F32),
            pltpu.VMEM((1, cols), F32),
            pltpu.VMEM((per, BLK, cols), BF16),
            pltpu.VMEM((bits, rank, mine), F32),
            pltpu.VMEM((bits, rank, mine), F32),
            pltpu.VMEM((tp, rank, mine), BF16),
            pltpu.VMEM((CHUNKS, per, tp, ROWS, rank), BF16),
            pltpu.VMEM((per, BLK, LANES), BF16),
            pltpu.VMEM((8, cols), F32),
            pltpu.VMEM((rank, cols), BF16),
            pltpu.VMEM((rank, cols), BF16),
            pltpu.VMEM((rank, cols), BF16),
            pltpu.VMEM((rank, cols), BF16),
            pltpu.VMEM((2, 1, cols), F32),
            pltpu.VMEM((2, 1, cols), F32),
            dma((tiles,)),
            dma((CHUNKS,)), dma((CHUNKS,)),
            dma((bits - 1, CHUNKS)), dma((bits - 1, CHUNKS)),
            dma((CHUNKS,)), dma((CHUNKS,)),
            dma((CHUNKS,)), dma((CHUNKS,)),
            dma((misc,)), dma((misc,)),
        ],
        compiler_params=pltpu.CompilerParams(
            collective_id=0, has_side_effects=True, vmem_limit_bytes=67043328
        ),
    )(
        tokens.reshape(2, CHUNKS, ROWS, width),
        routing,
        weight,
        down,
        up,
        mag.reshape(1, cols),
        cot.reshape(per, BLK, cols),
    )
    return out.reshape(mine, cols), ga, gb, gm.reshape(cols)


def solution(mesh):
    return jax.shard_map(
        functools.partial(body, mesh.shape["dp"], mesh.shape["tensor"]),
        mesh=mesh,
        in_specs=(
            P("dp", "tensor"),
            P(),
            P("tensor", "dp"),
            P(None, "tensor"),
            P(None, "dp"),
            P("dp"),
            P("tensor", "dp"),
        ),
        out_specs=(P("tensor", "dp"), P(None, "tensor"), P(None, "dp"), P("dp")),
        check_vma=False,
    )
```

```python
import functools
import math

import jax
import jax.numpy as jnp
from jax import lax
from jax.experimental import pallas as pl
from jax.experimental.pallas import tpu as pltpu
from jax.sharding import PartitionSpec as P

BLK = 128
ROWS = 16
CHUNKS = BLK // ROWS
HALVES = 2
UNITS = CHUNKS * HALVES
AHEAD = 2
LAG = 2
LANES = 128
MESH = pl.DeviceIdType.MESH
F32 = jnp.float32
BF16 = jnp.bfloat16


def mirrored(value, bits):
    result = 0
    for position in range(bits):
        result = result + (value // (1 << position)) % 2 * (1 << (bits - 1 - position))
    return result


def flipped(value, bit):
    return value + bit - 2 * bit * ((value // bit) % 2)


def dots(left, right, left_dim, right_dim):
    return lax.dot_general(
        left, right, (((left_dim,), (right_dim,)), ((), ())), preferred_element_type=F32
    )


def kernel(
    cfg,
    tok_in, routing, w_hbm, down, up, mag, cot,
    out, ga_out, gb_out, gm_out,
    w, raw, tok, part, near, pair, far, downp, sq, sq_near, sq_far, factor, norm, sg,
    rp, rp_in, rgt, rg, proj_down, gm_acc, gb_part, gb_near, gb_sum, gb_far, gb_all, gm_part, gm_in,
    d_part, d_near, d_pair, d_far,
    w_sem, s0_send, s0_recv, st_send, st_recv, nr_send, nr_recv, fr_send, fr_recv, ms_send, ms_recv,
    dn_send, dn_recv, df_send, df_recv,
):
    dp, tp, width, cols, rank, tile, tps = cfg
    bits = dp.bit_length() - 1
    per = dp // tp
    tiles = cols // tile
    scale = 1.0 / math.sqrt(rank)
    inverse = 1.0 / math.sqrt(dp * BLK)
    d = lax.axis_index("dp")
    t = lax.axis_index("tensor")
    core = t % 2
    side = t // 2
    t_near, t_far = flipped(t, 1), flipped(t, 2)
    hops = [flipped(d, dp >> (k + 1)) for k in range(bits)]

    def copy(src, dst, send, recv, target):
        return pltpu.make_async_remote_copy(
            src_ref=src, dst_ref=dst, send_sem=send, recv_sem=recv,
            device_id=target, device_id_type=MESH,
        )

    def to_dp(k):
        return {"dp": hops[k]}

    near_id, far_id = {"tensor": t_near}, {"tensor": t_far}

    def w_copy(n):
        at = pl.ds(pl.multiple_of(n * tile, tile), tile)
        return pltpu.make_async_copy(w_hbm.at[:, at], w.at[:, at], w_sem.at[n])

    half = width // HALVES

    def lanes(u):
        return pl.ds(pl.multiple_of(u % HALVES * half, half), half)

    def first(u):
        c = u // HALVES
        return copy(
            tok_in.at[:, c, :, lanes(u)], raw.at[c, :, :, lanes(u)],
            s0_send.at[u], s0_recv.at[u], to_dp(0),
        )

    def stage(k, u, owner):
        size = 1 << k
        base = mirrored(owner, bits) // size * size
        rows = pl.ds(pl.multiple_of(base * ROWS, ROWS), size * ROWS)
        here = tok.at[u // HALVES, rows, lanes(u)]
        return copy(here, here, st_send.at[k - 1, u], st_recv.at[k - 1, u], to_dp(k))

    def near_copy(c):
        start = (1 - core) * 2
        return copy(part.at[c, :, pl.ds(start, 2)], near.at[c], nr_send.at[c], nr_recv.at[c], near_id)

    def far_copy(c):
        return copy(pair.at[c], far.at[c], fr_send.at[c], fr_recv.at[c], far_id)

    def down_near(c):
        start = (1 - core) * 2
        return copy(d_part.at[c, :, pl.ds(start, 2)], d_near.at[c], dn_send.at[c], dn_recv.at[c], near_id)

    def down_far(c):
        return copy(d_pair.at[c], d_far.at[c], df_send.at[c], df_recv.at[c], far_id)

    def small(n, src, dst, target):
        return copy(src, dst, ms_send.at[n], ms_recv.at[n], target)

    sq1 = small(0, sq, sq_near, near_id)
    sq2 = small(1, sq_near, sq_far, far_id)
    rp_hops = [small(2 + k, rp.at[k], rp_in.at[k], to_dp(bits - 1 - k)) for k in range(bits)]
    n0 = 2 + bits
    rg1 = small(n0, rgt.at[t], rgt.at[t], near_id)
    rg1_in = small(n0, rgt.at[t_near], rgt.at[t_near], near_id)
    mine2 = pl.ds(side * 2, 2)
    theirs2 = pl.ds((1 - side) * 2, 2)
    rg2 = small(n0 + 1, rgt.at[mine2], rgt.at[mine2], far_id)
    rg2_in = small(n0 + 1, rgt.at[theirs2], rgt.at[theirs2], far_id)

    def each_tile(body):
        @pl.loop(0, tiles)
        def _(n):
            body(pl.ds(pl.multiple_of(n * tile, tile), tile))

    @pl.loop(0, tiles)
    def _(n):
        w_copy(n).start()

    barrier = pltpu.get_barrier_semaphore()
    for k in range(bits):
        pl.semaphore_signal(barrier, inc=1, device_id=to_dp(k), device_id_type=MESH)
    pl.semaphore_signal(barrier, inc=1, device_id=near_id, device_id_type=MESH)
    pl.semaphore_signal(barrier, inc=1, device_id=far_id, device_id_type=MESH)
    pl.semaphore_wait(barrier, bits + 2)

    for c in range(AHEAD):
        first(c).start()
    downp[...] = jnp.zeros_like(downp)
    downp[:rank, :] = down[...]
    gm_acc[...] = jnp.zeros_like(gm_acc)

    own_live = routing[d, 0] == d
    pair_live = routing[hops[0], 0] == hops[0]
    norm_last = (tiles + tps - 1) // tps - 1
    depth = 256

    def norm_tile(n):
        w_copy(n).wait()
        at = pl.ds(pl.multiple_of(n * tile, tile), tile)

        def add(r, total):
            rows = pl.ds(pl.multiple_of(r * depth, depth), depth)
            merged = w[rows, at].astype(F32) + scale * dots(down[:, rows], up[:, at], 0, 0)
            return total + jnp.sum((merged * merged).reshape(depth // 8, 8, tile), axis=0)

        total = lax.fori_loop(0, width // depth, add, jnp.zeros((8, tile), F32))
        sq[:, at] = jnp.sum(total, axis=0, keepdims=True)

    def gradient():
        def body(at):
            square = sq_near[:, at] + sq_far[:, at]
            size = jnp.maximum(jnp.sqrt(square), 0.5)
            ratio = mag[at].reshape(1, tile) / size
            norm[:, at] = size
            factor[:, at] = ratio
            for g in range(per):
                sg[g, :, at] = (cot[g, :, at].astype(F32) * ratio * inverse).astype(BF16)

        each_tile(body)
        for g in range(per):
            rp[0, :, g * BLK:(g + 1) * BLK] = dots(up[...], sg[g], 1, 1)
        rp_hops[0].start()

    def epilogue(c):
        mine = core * 2 + side
        rows = pl.ds(pl.multiple_of(c * ROWS, ROWS), ROWS)
        high = per * ROWS

        def total(at, wide):
            return (
                part[c, :, mine, :, at].astype(F32)
                + near[c, :, side, :, at].astype(F32)
                + far[c, :, :, at].astype(F32)
            ).reshape(high, wide)

        lhs = proj_down[:, rows, :].reshape(high, LANES)[:, :rank]

        def body(at):
            pre = total(at, tile) + scale * jnp.dot(lhs, up[:, at], preferred_element_type=F32)
            out[:, rows, at] = (pre * factor[:, at]).astype(BF16).reshape(per, ROWS, tile)
            both = cot[:, rows, at].astype(F32).reshape(high, tile) * pre
            gm_acc[:, at] += jnp.sum(both.reshape(high // 8, 8, tile), axis=0)

        each_tile(body)

    def when(condition, action):
        pl.when(condition)(action)

    grad_at = norm_last + 2
    gap = max(1, (UNITS + 1 - grad_at) // bits)
    parts = -(-tiles // 2)

    @pl.loop(0, UNITS + LAG * (bits - 1) + 2)
    def _(u):
        when(u + AHEAD < UNITS, lambda: first(u + AHEAD).start())

        @pl.when(u < UNITS)
        def _():
            first(u).wait_recv()
            c = u // HALVES
            at = lanes(u)
            own_at = pl.ds(pl.multiple_of(mirrored(d, bits) * ROWS, ROWS), ROWS)
            pair_at = pl.ds(pl.multiple_of(mirrored(hops[0], bits) * ROWS, ROWS), ROWS)
            tok[c, own_at, at] = jnp.where(own_live, tok_in[0, c, :, at], raw[c, 1, :, at])
            tok[c, pair_at, at] = jnp.where(pair_live, raw[c, 0, :, at], tok_in[1, c, :, at])
            stage(1, u, d).start()

        for k in range(1, bits):
            v = u - LAG * k

            @pl.when((v >= 0) & (v < UNITS))
            def _():
                stage(k, v, hops[k]).wait_recv()
                if k < bits - 1:
                    stage(k + 1, v, d).start()

        @pl.when(u <= norm_last)
        def _():
            for e in range(tps):
                n = u * tps + e
                when(n < tiles, lambda: norm_tile(n))

        when(u == norm_last, lambda: sq1.start())

        @pl.when(u == norm_last + 1)
        def _():
            sq1.wait()
            sq_near[...] = sq_near[...] + sq[...]
            sq2.start()

        @pl.when(u == grad_at)
        def _():
            sq2.wait()
            gradient()

        for k in range(bits):
            @pl.when(u == grad_at + gap * (k + 1))
            def _():
                rp_hops[k].wait()
                merged = rp[k] + rp_in[k]
                if k < bits - 1:
                    rp[k + 1] = merged
                    rp_hops[k + 1].start()
                else:
                    rgt[t] = merged.astype(BF16)
                    rg1.start()

        @pl.when(u == grad_at + gap * bits + 1)
        def _():
            rg1.wait_send()
            rg1_in.wait_recv()
            rg2.start()

        m = u - LAG * (bits - 1) - 1
        j = m // 2
        even = m % 2 == 0

        @pl.when((m >= 2) & even)
        def _():
            c = j - 1
            near_copy(c).wait_recv()
            other = core * 2 + 1 - side

            def body(at):
                pair[c, :, :, at] = (
                    part[c, :, other, :, at].astype(F32)
                    + near[c, :, 1 - side, :, at].astype(F32)
                ).astype(BF16)

            each_tile(body)
            far_copy(c).start()

        @pl.when((m >= 0) & even & (j < CHUNKS))
        def _():
            d_part[j] = dots(tok[j], downp[...], 1, 1).astype(BF16).reshape(per, tp, ROWS, LANES)
            down_near(j).start()

        @pl.when((m >= 0) & (j < CHUNKS))
        def _():
            lhs = tok.at[j]
            begin = (m % 2) * parts

            @pl.loop(0, parts)
            def _(e):
                n = begin + e

                @pl.when(n < tiles)
                def _():
                    at = pl.ds(pl.multiple_of(n * tile, tile), tile)
                    prod = jnp.dot(lhs[...], w[:, at], preferred_element_type=F32)
                    part[j, :, :, :, at] = prod.astype(BF16).reshape(per, tp, ROWS, tile)

        @pl.when((m >= 0) & (m % 2 == 1) & (j < CHUNKS))
        def _():
            near_copy(j).start()
            down_near(j).wait_recv()
            d_pair[j] = (
                d_part[j, :, core * 2 + 1 - side].astype(F32) + d_near[j, :, 1 - side].astype(F32)
            ).astype(BF16)
            down_far(j).start()

        @pl.when((m >= 2) & even)
        def _():
            c = j - 1
            down_far(c).wait_recv()
            rows = pl.ds(pl.multiple_of(c * ROWS, ROWS), ROWS)
            proj_down[:, rows, :] = (
                d_part[c, :, core * 2 + side].astype(F32)
                + d_near[c, :, side].astype(F32)
                + d_far[c].astype(F32)
            ).astype(BF16)

        @pl.when((m >= 5) & (m % 2 == 1))
        def _():
            c = (m - 5) // 2
            far_copy(c).wait_recv()
            epilogue(c)

    n1 = n0 + 2
    share = rank // 2
    gb1 = small(n1, gb_part.at[1 - core], gb_near, near_id)
    gb2 = small(n1 + 1, gb_sum, gb_far, far_id)
    gb3 = small(n1 + 4, gb_all.at[core], gb_all.at[core], near_id)
    gb3_in = small(n1 + 4, gb_all.at[1 - core], gb_all.at[1 - core], near_id)
    gm1 = small(n1 + 2, gm_part.at[0], gm_in.at[0], near_id)
    gm2 = small(n1 + 3, gm_part.at[1], gm_in.at[1], far_id)
    live = proj_down[...].reshape(per * BLK, LANES)[:, :rank]

    def ends(at):
        gb_part[:, :, at] = (
            scale * dots(live, sg[:, :, at].reshape(per * BLK, tile), 0, 0)
        ).astype(BF16).reshape(2, share, tile)

    each_tile(ends)
    gb1.start()

    far_copy(CHUNKS - 2).wait_recv()
    epilogue(CHUNKS - 2)

    gb1.wait()

    def sums(at):
        gb_sum[:, at] = (gb_part[core, :, at].astype(F32) + gb_near[:, at].astype(F32)).astype(BF16)

    each_tile(sums)
    gb2.start()

    rg2.wait_send()
    rg2_in.wait_recv()
    for s in range(tp):
        turned = rgt[s].astype(F32).T.astype(BF16)
        spot = s % 2 * 2 + s // 2
        for g in range(per):
            rg[:, g, spot] = turned[g * BLK:(g + 1) * BLK].reshape(CHUNKS, ROWS, rank)

    wide = min(512, width)

    @pl.loop(0, width // wide)
    def _(n):
        at = pl.ds(pl.multiple_of(n * wide, wide), wide)

        def add(c, total):
            return total + dots(rg[c].reshape(dp * ROWS, rank), tok[c, :, at], 0, 0)

        ga_out[:, at] = scale * lax.fori_loop(0, CHUNKS, add, jnp.zeros((rank, wide), F32))

    far_copy(CHUNKS - 1).wait_recv()
    epilogue(CHUNKS - 1)

    def shares(at):
        gm_part[0, :, at] = (
            jnp.sum(gm_acc[:, at], axis=0, keepdims=True) / norm[:, at] * inverse
        )

    each_tile(shares)
    gm1.start()
    gm1.wait()
    gm_part[1] = gm_part[0] + gm_in[0]
    gm2.start()
    gb2.wait()

    def last(at):
        gb_all[core, :, at] = gb_sum[:, at].astype(F32) + gb_far[:, at].astype(F32)

    each_tile(last)
    gb3.start()
    gm2.wait()
    gm_out[...] = (gm_part[1] + gm_in[1]).reshape(cols)
    gb3.wait_send()
    gb3_in.wait_recv()
    gb_out[...] = gb_all[...].reshape(rank, cols)

    @pl.loop(0, UNITS)
    def _(u):
        first(u).wait_send()
        for k in range(1, bits):
            stage(k, u, d).wait_send()

    @pl.loop(0, CHUNKS)
    def _(c):
        near_copy(c).wait_send()
        far_copy(c).wait_send()
        down_near(c).wait_send()
        down_far(c).wait_send()


def body(dp, tp, tokens, routing, weight, down, up, mag, cot):
    width, cols = weight.shape
    rank = down.shape[0]
    per = dp // tp
    bits = dp.bit_length() - 1
    tile = next(size for size in (512, 256, 128) if cols % size == 0)
    tiles = cols // tile
    tps = -(-tiles // (bits + 1))
    cfg = (dp, tp, width, cols, rank, tile, tps)
    ext = cols
    vmem = pl.BlockSpec(memory_space=pltpu.VMEM)
    dma = pltpu.SemaphoreType.DMA
    mine = per * BLK
    misc = bits + 9
    out, ga, gb, gm = pl.pallas_call(
        functools.partial(kernel, cfg),
        out_shape=(
            jax.ShapeDtypeStruct((per, BLK, cols), BF16),
            jax.ShapeDtypeStruct((rank, width), F32),
            jax.ShapeDtypeStruct((rank, cols), F32),
            jax.ShapeDtypeStruct((cols,), F32),
        ),
        in_specs=[
            vmem,
            pl.BlockSpec(memory_space=pltpu.SMEM),
            pl.BlockSpec(memory_space=pl.ANY),
            vmem, vmem, vmem, vmem,
        ],
        out_specs=(vmem, vmem, vmem, vmem),
        scratch_shapes=[
            pltpu.VMEM((width, cols), BF16),
            pltpu.VMEM((CHUNKS, 2, ROWS, width), BF16),
            pltpu.VMEM((CHUNKS, dp * ROWS, width), BF16),
            pltpu.VMEM((CHUNKS, per, tp, ROWS, ext), BF16),
            pltpu.VMEM((CHUNKS, per, 2, ROWS, ext), BF16),
            pltpu.VMEM((CHUNKS, per, ROWS, ext), BF16),
            pltpu.VMEM((CHUNKS, per, ROWS, ext), BF16),
            pltpu.VMEM((LANES, width), BF16),
            pltpu.VMEM((1, cols), F32),
            pltpu.VMEM((1, cols), F32),
            pltpu.VMEM((1, cols), F32),
            pltpu.VMEM((1, cols), F32),
            pltpu.VMEM((1, cols), F32),
            pltpu.VMEM((per, BLK, cols), BF16),
            pltpu.VMEM((bits, rank, mine), F32),
            pltpu.VMEM((bits, rank, mine), F32),
            pltpu.VMEM((tp, rank, mine), BF16),
            pltpu.VMEM((CHUNKS, per, tp, ROWS, rank), BF16),
            pltpu.VMEM((per, BLK, LANES), BF16),
            pltpu.VMEM((8, cols), F32),
            pltpu.VMEM((2, rank // 2, cols), BF16),
            pltpu.VMEM((rank // 2, cols), BF16),
            pltpu.VMEM((rank // 2, cols), BF16),
            pltpu.VMEM((rank // 2, cols), BF16),
            pltpu.VMEM((2, rank // 2, cols), F32),
            pltpu.VMEM((2, 1, cols), F32),
            pltpu.VMEM((2, 1, cols), F32),
            pltpu.VMEM((CHUNKS, per, tp, ROWS, LANES), BF16),
            pltpu.VMEM((CHUNKS, per, 2, ROWS, LANES), BF16),
            pltpu.VMEM((CHUNKS, per, ROWS, LANES), BF16),
            pltpu.VMEM((CHUNKS, per, ROWS, LANES), BF16),
            dma((tiles,)),
            dma((UNITS,)), dma((UNITS,)),
            dma((bits - 1, UNITS)), dma((bits - 1, UNITS)),
            dma((CHUNKS,)), dma((CHUNKS,)),
            dma((CHUNKS,)), dma((CHUNKS,)),
            dma((misc,)), dma((misc,)),
            dma((CHUNKS,)), dma((CHUNKS,)),
            dma((CHUNKS,)), dma((CHUNKS,)),
        ],
        compiler_params=pltpu.CompilerParams(
            collective_id=0, has_side_effects=True, vmem_limit_bytes=67043328
        ),
    )(
        tokens.reshape(2, CHUNKS, ROWS, width),
        routing,
        weight,
        down,
        up,
        mag,
        cot.reshape(per, BLK, cols),
    )
    return out.reshape(mine, cols), ga, gb, gm


def solution(mesh):
    return jax.shard_map(
        functools.partial(body, mesh.shape["dp"], mesh.shape["tensor"]),
        mesh=mesh,
        in_specs=(
            P("dp", "tensor"),
            P(),
            P("tensor", "dp"),
            P(None, "tensor"),
            P(None, "dp"),
            P("dp"),
            P("tensor", "dp"),
        ),
        out_specs=(P("tensor", "dp"), P(None, "tensor"), P(None, "dp"), P("dp")),
        check_vma=False,
    )
```
